32 devices in a mesh: freq: 8 (over z, y), col: 4 (over x, core).
Axes of the slice: x: 2, y: 2, z: 4, core: 2. Of those that a mesh axis runs over, the one named last changes fastest.
Arguments:
- traces: bfloat16 [16, 512, 64, 512], P('col', 'freq'), may hold values from -6 to 6
- left_factors: bfloat16 [32, 16, 16, 16, 512], P('freq', None, 'col'), may hold values from -0.5 to 0.5
- right_factors: bfloat16 [32, 16, 16, 16, 512], P('freq', None, 'col'), may hold values from -0.25 to 0.25
- tile_ranks: int32 [32, 16, 16], P('freq', None, 'col'), may hold values from 1 to 16, as said below
Outputs:
- modelled: bfloat16 [16, 512, 64, 512], P('col', 'freq')
The draws below stay inside these ranges and needn't reach their ends.
Inputs may be any that keep to these rules, and one draw needn't show every extreme that they name: `tile_ranks`: the rank of each kernel tile; factor rows at or past it are not part of the kernel. 16 is reached by some tile in every draw.
All inputs are finite; a program needn't handle non-finite values.
Results may differ from the reference program's by a relative error of at most 0.0072.
Values may be sent and summed in bfloat16 or wider, within the bound.
No kernel may reach another device: no remote copies, remote signals or barrier semaphores. Data moves between devices by JAX's collectives and lax.ppermute only.
A program may use at most 128 MiB of HBM per device.

```python
import jax
import jax.numpy as jnp
from jax import lax

NT = 512
TS = 512
RMAX = 16
NF = 32
NVB = 64
RT = 16
CT = 16


def draw_tile_ranks(key, part):
    base_key = jax.random.fold_in(key, 11)
    first_key, second_key, third_key = jax.random.split(base_key, 3)
    freq_index = jnp.arange(NF, dtype=jnp.int32)[:, None, None]
    low_cap = max(RMAX // 4, 1)
    rank_caps = low_cap + (RMAX - low_cap) * freq_index // max(NF - 1, 1)
    raw_draws = jax.random.randint(first_key, (NF, RT, CT), 0, 1 << 20)
    ranks_drawn = 1 + raw_draws % rank_caps
    chosen_freq = jax.random.randint(second_key, (), NF // 2, NF)
    chosen_tile = jax.random.randint(third_key, (), 0, RT * CT)
    tile_index = jnp.arange(RT * CT, dtype=jnp.int32).reshape(1, RT, CT)
    chosen_mask = (freq_index == chosen_freq) & (tile_index == chosen_tile)
    return jnp.where(chosen_mask, RMAX, ranks_drawn).astype(jnp.int32)


def strengthened(values, stream_key, source, target, parts, factor):
    owner, partner = [(jnp.arange(values.shape[position]) // (values.shape[position] // parts)).reshape([-1 if axis == position else 1 for axis in range(values.ndim)]) for position in (source, target)]
    chosen = jax.random.permutation(stream_key, parts)[partner]
    strong = (owner == chosen) | (owner == (partner + parts // 2) % parts)
    return jnp.where(strong, factor * values, values)


def shard_levels(stream_key, extent, pieces, least, high):
    level = 1.0
    for position, blocks in pieces:
        steps = jax.random.uniform(jax.random.fold_in(jax.random.fold_in(stream_key, 6), position), (blocks,), jnp.float32, least / len(pieces), high / len(pieces))
        level = level * jnp.repeat(jnp.exp(steps), extent[position] // blocks).reshape((-1,) + (1,) * (len(extent) - 1 - position))
    return level


def normal_values(stream_key, shape, spread, limit, cuts=(), held_as=jnp.bfloat16):
    level = shard_levels(stream_key, shape, cuts, -0.22, 0.18) if cuts else 1.0
    drawn = jax.random.normal(stream_key, shape, jnp.float32) * spread * level
    return jnp.minimum(jnp.maximum(drawn, -limit), limit).astype(held_as)


def noise_with(key, dims, spread, limit, shards, heavy, kind=jnp.bfloat16):
    array = spread * jax.random.normal(key, dims, jnp.float32)
    if shards:
        array = array * shard_levels(key, dims, shards, -0.22, 0.18)
    return jnp.clip(strengthened(array, jax.random.fold_in(key, 3), *heavy), -limit, limit).astype(kind)


def setup_inputs(seed: int = 0) -> dict:
    keys = jax.random.split(jax.random.key(seed), 5)
    return {
        "traces": normal_values(keys[0], (CT, TS, NVB, NT), 1.0, 6.0, ((0, 4), (1, 8))),
        "left_factors": noise_with(keys[1], (NF, RT, CT, RMAX, TS), (RMAX * CT) ** -0.5, 0.5, ((0, 8), (2, 4)), (2, 1, 4, 2.0)),
        "right_factors": normal_values(keys[2], (NF, RT, CT, RMAX, TS), TS ** -0.5, 0.25, ((0, 8), (2, 4))),
        "tile_ranks": draw_tile_ranks(jax.random.fold_in(keys[4], 71), 0),
    }


def hartley_table(time_count, freq_count):
    times = jnp.arange(time_count, dtype=jnp.int32)
    freqs = jnp.arange(freq_count, dtype=jnp.int32)
    phase = times[:, None] * freqs[None, :] % time_count
    angle = 2.0 * jnp.pi / time_count * phase.astype(jnp.float32)
    scale = jnp.sqrt(jnp.float32(time_count))
    return ((jnp.cos(angle) + jnp.sin(angle)) / scale).astype(jnp.bfloat16)

def reference(traces, left_factors, right_factors, tile_ranks):
    cas_table = hartley_table(NT, NF).astype(jnp.float32)

    def forward(tile):
        return jnp.einsum('swt,tk->kws', tile.astype(jnp.float32), cas_table).astype(jnp.bfloat16)
    spectra = jnp.moveaxis(lax.map(forward, traces), 1, 0)

    def apply_kernel(operands):
        spectrum, right_tiles, left_tiles, rank_tiles = operands
        coeffs = jnp.einsum('cws,rcks->rwck', spectrum.astype(jnp.float32), right_tiles.astype(jnp.float32))
        kept_mask = jnp.arange(RMAX, dtype=jnp.int32)[None, None, None, :] < rank_tiles[:, None, :, None]
        coeffs = jnp.where(kept_mask, coeffs, jnp.float32(0.0)).astype(jnp.bfloat16)
        summed = jnp.einsum('rwck,rcks->rws', coeffs.astype(jnp.float32), left_tiles.astype(jnp.float32))
        return summed.astype(jnp.bfloat16)
    synthesis = lax.map(apply_kernel, (spectra, right_factors, left_factors, tile_ranks))
    synthesis = jnp.moveaxis(synthesis, 1, 0)

    def inverse(block):
        return jnp.einsum('kws,tk->swt', block.astype(jnp.float32), cas_table).astype(jnp.bfloat16)
    return lax.map(inverse, synthesis)
```

```python
import functools

import jax
import jax.numpy as jnp
import numpy as np
from jax import lax
from jax.experimental import pallas as pl
from jax.experimental.pallas import tpu as pltpu
from jax.sharding import PartitionSpec as P

LANES = 128
WIDE = 58 << 20
ROWS = 16


def hartley_table(time_count, freq_count):
    phase = np.arange(time_count)[:, None] * np.arange(freq_count)[None, :] % time_count
    angle = np.float32(2.0 * np.pi / time_count) * phase.astype(np.float32)
    table = (np.cos(angle) + np.sin(angle)) / np.sqrt(np.float32(time_count))
    return table.astype(np.float32).astype(jnp.bfloat16)


def forward_kernel(x_ref, cas_ref, *refs, shares, depth, group):
    spectra, (buffer, held, arrived) = refs[:shares], refs[shares:]
    steps, pack, count, _, _ = buffer.shape
    all_freqs = cas_ref.shape[0]
    freqs = all_freqs // shares
    across = x_ref.shape[1] // count
    place = lax.axis_index("freq")

    def copies(step):
        first = pl.multiple_of(step % across * count, count)
        return [
            pltpu.make_async_copy(
                x_ref.at[step // across * pack + c, pl.ds(first, count)], buffer.at[step, c], arrived.at[step, c]
            )
            for c in range(pack)
        ]

    for step in range(min(depth, steps)):
        for copy in copies(step):
            copy.start()

    def body(step, carry):
        for copy in copies(step):
            copy.wait()

        @pl.when(step + depth < steps)
        def _():
            for copy in copies(step + depth):
                copy.start()

        for s in range(0, count, group):
            rows = jnp.concatenate([buffer[step, c, s + i] for i in range(group) for c in range(pack)], axis=0)
            product = lax.dot_general(
                cas_ref[...], rows, (((1,), (1,)), ((), ())), preferred_element_type=jnp.float32
            )
            for i in range(group):
                held[(s + i) * all_freqs : (s + i + 1) * all_freqs, :] = product[:, i * LANES : (i + 1) * LANES]
        first = pl.multiple_of(step % across * count, count)
        for shift in range(shares):
            low = lax.rem(place + shift, shares) * freqs
            for k in range(freqs):
                spectra[shift][k, step // across, pl.ds(first, count), :] = held[
                    pl.ds(low + k, count, stride=all_freqs), :
                ].astype(jnp.bfloat16)
        return carry

    lax.fori_loop(0, steps, body, 0)


def forward(traces, cas, shares):
    tiles, sources, waves, times = traces.shape
    all_freqs = cas.shape[0]
    freqs = all_freqs // shares
    pack = LANES // waves
    count = min(ROWS, sources)
    steps = tiles // pack * (sources // count)
    vmem = pl.BlockSpec(memory_space=pltpu.VMEM)
    return pl.pallas_call(
        functools.partial(forward_kernel, shares=shares, depth=4, group=4),
        out_shape=[jax.ShapeDtypeStruct((freqs, tiles // pack, sources, LANES), jnp.bfloat16)] * shares,
        in_specs=[pl.BlockSpec(memory_space=pltpu.HBM), vmem],
        out_specs=[vmem] * shares,
        scratch_shapes=[
            pltpu.VMEM((steps, pack, count, waves, times), jnp.bfloat16),
            pltpu.VMEM((count * all_freqs, LANES), jnp.float32),
            pltpu.SemaphoreType.DMA((steps, pack)),
        ],
        cost_estimate=pl.CostEstimate(
            flops=2 * traces.size * all_freqs, bytes_accessed=2 * traces.size, transcendentals=0
        ),
        name="forward",
    )(traces, cas)


def stage_kernel(*refs, count, pieces):
    operands, outputs, arrived = refs[:count], refs[count:-1], refs[-1]
    me = lax.axis_index("col")
    copies = [
        pltpu.make_async_copy(
            operands[operand] if take is None else operands[operand].at[:, pl.ds(take(me), wide)],
            outputs[output] if put is None else outputs[output].at[:, put],
            arrived.at[i],
        )
        for i, (operand, output, take, wide, put) in enumerate(pieces)
    ]
    for copy in copies:
        copy.start()
    for copy in copies:
        copy.wait()


def stage(operands, shapes, pieces, grant):
    return pl.pallas_call(
        functools.partial(stage_kernel, count=len(operands), pieces=pieces),
        out_shape=[jax.ShapeDtypeStruct(shape, jnp.bfloat16) for shape in shapes],
        in_specs=[pl.BlockSpec(memory_space=pltpu.HBM)] * len(operands),
        out_specs=[pl.BlockSpec(memory_space=pltpu.VMEM)] * len(shapes),
        scratch_shapes=[pltpu.SemaphoreType.DMA((len(pieces),))],
        cost_estimate=pl.CostEstimate(flops=1 << 28, bytes_accessed=1 << 22, transcendentals=0),
        compiler_params=pltpu.CompilerParams(vmem_limit_bytes=grant),
        name="stage",
    )(*operands)


def coeff_kernel(ranks_ref, right_ref, *refs, shares, owners, inner):
    spectra, direct = refs[:shares], refs[shares : shares + owners]
    paired, (spec_ref, rows_ref, right_held, own_held, arrived) = refs[shares + owners : -5], refs[-5:]
    freqs, receivers, tiles, ranks, sources = right_ref.shape
    own = pltpu.make_async_copy(spectra[0], own_held, arrived.at[freqs])
    own.start()
    for k in range(freqs):
        pltpu.make_async_copy(right_ref.at[k], right_held.at[k], arrived.at[k]).start()
    spectra = [own_held] + list(spectra[1:])
    pairs, each = spectra[0].shape[1:3]
    pack = tiles // pairs
    waves = LANES // pack
    me, place = lax.axis_index("col"), lax.axis_index("freq")
    lane_tile = lax.broadcasted_iota(jnp.int32, (ranks, LANES), 1) // waves
    rank_row = lax.broadcasted_iota(jnp.int32, (ranks, LANES), 0)
    per_owner = receivers // owners

    own.wait()

    def body(k, carry):
        pltpu.make_async_copy(right_ref.at[k], right_held.at[k], arrived.at[k]).wait()
        for pair in range(pairs):
            for shift in range(shares):
                first = pl.multiple_of(lax.rem(place + shares - shift, shares) * each, each)
                spec_ref[pair, pl.ds(first, each), :] = spectra[shift][k, pair]
        for pair in range(pairs):
            product = [
                jnp.dot(
                    right_held[k, :, pair * pack + h].reshape(receivers * ranks, sources),
                    spec_ref[pair],
                    preferred_element_type=jnp.float32,
                )
                for h in range(pack)
            ]
            for r in range(receivers):
                entry = (k * receivers + r) * tiles + pair * pack
                kept = product[0][r * ranks : (r + 1) * ranks]
                limit = jnp.full((ranks, LANES), ranks_ref[entry], jnp.int32)
                for h in range(1, pack):
                    here = lane_tile == h
                    kept = jnp.where(here, product[h][r * ranks : (r + 1) * ranks], kept)
                    limit = jnp.where(here, ranks_ref[entry + h], limit)
                kept = jnp.where(rank_row < limit, kept, 0.0)
                rows_ref[pair, r] = kept.astype(jnp.bfloat16)
            for shift in range(owners):
                first = lax.rem(me + shift, owners) * per_owner
                for i in range(pack):
                    direct[shift][k, pair, i * ranks : (i + 1) * ranks, :] = rows_ref[pair, first + i]
            for side in range(inner):
                core = lax.rem(me + side, inner)
                for outer in range(owners // inner):
                    first = (outer * inner + core) * per_owner + pack
                    for i in range(pack):
                        paired[side][k, outer, pair, i * ranks : (i + 1) * ranks, :] = rows_ref[pair, first + i]
        return carry

    lax.fori_loop(0, freqs, body, 0)


def coefficients(ranks, spectra, right, owners, inner):
    freqs, receivers, tiles, rank_count, sources = right.shape
    shares = len(spectra)
    pairs = spectra[0].shape[1]
    rows = tiles // pairs * rank_count
    outer = owners // inner
    vmem, smem = pl.BlockSpec(memory_space=pltpu.VMEM), pl.BlockSpec(memory_space=pltpu.SMEM)
    anywhere = pl.BlockSpec(memory_space=pl.ANY)
    return pl.pallas_call(
        functools.partial(coeff_kernel, shares=shares, owners=owners, inner=inner),
        out_shape=[jax.ShapeDtypeStruct((freqs, pairs, rows, LANES), jnp.bfloat16)] * owners
        + [jax.ShapeDtypeStruct((freqs, outer, pairs, rows, LANES), jnp.bfloat16)] * inner,
        in_specs=[smem, anywhere, anywhere] + [vmem] * (shares - 1),
        out_specs=[vmem] * (owners + inner),
        scratch_shapes=[
            pltpu.VMEM((pairs, sources, LANES), jnp.bfloat16),
            pltpu.VMEM((pairs, receivers, rank_count, LANES), jnp.bfloat16),
            pltpu.VMEM(right.shape, jnp.bfloat16),
            pltpu.VMEM(spectra[0].shape, jnp.bfloat16),
            pltpu.SemaphoreType.DMA((freqs + 1,)),
        ],
        cost_estimate=pl.CostEstimate(
            flops=2 * right.size * LANES, bytes_accessed=2 * right.size, transcendentals=0
        ),
        compiler_params=pltpu.CompilerParams(vmem_limit_bytes=WIDE),
        name="coefficients",
    )(ranks.reshape(-1), right, *spectra)


def synthesis_kernel(*refs, count, chip, added):
    coeff_refs, left_refs = refs[:count], refs[count : 2 * count]
    freqs = left_refs[0].shape[0]
    pack, tiles, ranks, sources = left_refs[0].shape[-4:]
    waves = LANES // pack
    place = lax.axis_index("freq")
    here = None if chip is None else chip(lax.axis_index("col"))
    outputs = refs[2 * count + added :]
    turned = len(outputs) > 1
    if turned:
        outputs, turned_ref = outputs[:-1], outputs[-1]
        shares = len(outputs)
        each = sources // shares

    def pick(ref, k, rank):
        if len(ref.shape) == rank + 1:
            return ref.at[k]
        return ref.at[k, ref.shape[1] - 1 if here is None else here]

    for k in range(freqs):
        parts = []
        for r in range(pack):
            weights = jnp.concatenate(
                [
                    pick(ref, k, 3)[
                        c // pack, r * ranks : (r + 1) * ranks, c % pack * waves : (c % pack + 1) * waves
                    ]
                    for ref in coeff_refs
                    for c in range(tiles)
                ],
                axis=0,
            )
            left = jnp.concatenate([pick(ref, k, 4)[r].reshape(tiles * ranks, sources) for ref in left_refs], axis=0)
            part = lax.dot_general(weights, left, (((0,), (0,)), ((), ())), preferred_element_type=jnp.float32)
            if added:
                part = part + refs[2 * count][k, r].astype(jnp.float32)
            parts.append(part.astype(jnp.bfloat16))
        if turned:
            turned_ref[k] = jnp.concatenate(parts, axis=0).T
            for shift in range(shares):
                first = pl.multiple_of(lax.rem(place + shift, shares) * each, each)
                outputs[shift][k] = turned_ref[k, pl.ds(first, each), :]
        else:
            for r in range(pack):
                outputs[0][k, r] = parts[r]


def synthesis(coeffs, lefts, added, shares, waves, chip):
    pack = LANES // waves
    freqs = coeffs[0].shape[0]
    tiles, rank_count, sources = lefts[0].shape[-3:]
    vmem = pl.BlockSpec(memory_space=pltpu.VMEM)
    if shares:
        out_shape = [jax.ShapeDtypeStruct((freqs, sources // shares, LANES), jnp.bfloat16)] * shares
        scratch = [pltpu.VMEM((freqs, sources, LANES), jnp.bfloat16)]
    else:
        out_shape = [jax.ShapeDtypeStruct((freqs, pack, waves, sources), jnp.bfloat16)]
        scratch = []
    extra = [] if added is None else [added]
    flops = 2 * freqs * pack * waves * sources * tiles * rank_count * len(coeffs)
    return pl.pallas_call(
        functools.partial(synthesis_kernel, count=len(coeffs), chip=chip, added=len(extra)),
        out_shape=out_shape,
        in_specs=[vmem] * (2 * len(coeffs) + len(extra)),
        out_specs=[vmem] * len(out_shape),
        scratch_shapes=scratch,
        cost_estimate=pl.CostEstimate(flops=flops, bytes_accessed=flops // waves, transcendentals=0),
        compiler_params=pltpu.CompilerParams(vmem_limit_bytes=8 << 20),
        name="synthesis",
    )(*coeffs, *lefts, *extra)


def inverse_kernel(cas_ref, *refs, shares, group):
    syn_refs = refs[:shares]
    out_ref, buffer, held, left = refs[-4:]
    steps, pack, count, waves, _ = buffer.shape
    freqs = cas_ref.shape[0]
    rows = freqs // shares * count
    place = lax.axis_index("freq")

    def copies(step):
        first = pl.multiple_of(step * count, count)
        return [
            pltpu.make_async_copy(
                buffer.at[step, r], out_ref.at[group * pack + r, pl.ds(first, count)], left.at[step, r]
            )
            for r in range(pack)
        ]

    def body(step, carry):
        first = pl.multiple_of(step * count, count)
        for shift in range(shares):
            low = pl.multiple_of(lax.rem(place + shares - shift, shares) * rows, rows)
            held[pl.ds(low, rows), :] = (
                syn_refs[shift][:, pl.ds(first, count), :].astype(jnp.float32).reshape(rows, LANES)
            )
        for s in range(count):
            weights = held[pl.ds(s, freqs, stride=count), :].astype(jnp.bfloat16)
            block = lax.dot_general(
                weights, cas_ref[...], (((0,), (0,)), ((), ())), preferred_element_type=jnp.float32
            ).astype(jnp.bfloat16)
            for r in range(pack):
                buffer[step, r, s] = block[r * waves : (r + 1) * waves]
        for copy in copies(step):
            copy.start()
        return carry

    lax.fori_loop(0, steps, body, 0)
    for step in range(steps):
        for copy in copies(step):
            copy.wait()


def inverse(synthesised, cas, waves, group, groups, partial):
    shares = len(synthesised)
    _, sources, _ = synthesised[0].shape
    freqs, times = cas.shape
    pack = LANES // waves
    count = min(ROWS, sources)
    steps = sources // count
    vmem = pl.BlockSpec(memory_space=pltpu.VMEM)
    extra = [] if partial is None else [partial]
    return pl.pallas_call(
        functools.partial(inverse_kernel, shares=shares, group=group),
        out_shape=jax.ShapeDtypeStruct((groups * pack, sources, waves, times), jnp.bfloat16),
        in_specs=[vmem] + [vmem] * shares + [pl.BlockSpec(memory_space=pltpu.HBM)] * len(extra),
        out_specs=pl.BlockSpec(memory_space=pltpu.HBM),
        scratch_shapes=[
            pltpu.VMEM((steps, pack, count, waves, times), jnp.bfloat16),
            pltpu.VMEM((freqs * count, LANES), jnp.float32),
            pltpu.SemaphoreType.DMA((steps, pack)),
        ],
        input_output_aliases={1 + shares: 0} if extra else {},
        cost_estimate=pl.CostEstimate(
            flops=2 * sources * LANES * times * freqs,
            bytes_accessed=2 * sources * LANES * times,
            transcendentals=0,
        ),
        compiler_params=pltpu.CompilerParams(vmem_limit_bytes=14 << 20),
        name="inverse",
    )(cas, *synthesised, *extra)


def shards(traces, left_factors, right_factors, tile_ranks):
    shares, owners = lax.axis_size("freq"), lax.axis_size("col")
    inner = 2
    outer = owners // inner
    freq_local, receivers = left_factors.shape[:2]
    tile = left_factors.shape[2:]
    waves = traces.shape[2]
    pack = LANES // waves
    per_owner = receivers // owners
    groups = per_owner // pack
    cas = jnp.asarray(hartley_table(traces.shape[3], freq_local * shares).T)

    def shifted(block, shift, axis, size):
        return lax.ppermute(block, axis, [(i, (i + shift) % size) for i in range(size)])

    def exchanged(blocks, axis):
        size = len(blocks)
        arrived = [blocks[0]] + [None] * (size - 1)
        for shift in start_order(size):
            arrived[shift] = shifted(blocks[shift], shift, axis, size)
        return arrived

    def swapped(block, bit):
        return lax.ppermute(block, "col", [(i, i ^ bit) for i in range(owners)])

    made = list(forward(traces, cas, shares))

    def direct_first(shift):
        return lambda me: lax.rem(me + shift, owners) * per_owner

    def paired_first(side, chip):
        return lambda me: (chip * inner + lax.rem(me + side, inner)) * per_owner + pack

    direct_shape = (freq_local, pack) + tile
    paired_shape = (freq_local, outer, pack) + tile
    left_direct = stage(
        [left_factors],
        [direct_shape] * (owners - 1),
        [(0, shift - 1, direct_first(shift), pack, None) for shift in range(1, owners)],
        WIDE,
    )
    left_own, left_other = stage(
        [left_factors],
        [(freq_local, outer + 1, pack) + tile, paired_shape],
        [(0, side, paired_first(side, chip), pack, chip) for side in (1, 0) for chip in range(outer)]
        + [(0, 0, direct_first(0), pack, outer)],
        12 << 20,
    )
    spectra = exchanged(made, "freq")
    left_direct = exchanged([left_own] + list(left_direct), "col")
    left_paired = [left_own, swapped(left_other, 1)]

    made = list(coefficients(tile_ranks, spectra, right_factors, owners, inner))
    paired = [made[-2], swapped(made[-1], 1)]
    direct = exchanged(made[:owners], "col")
    (sent,) = synthesis(paired, left_paired, None, 0, waves, lambda me: (me ^ inner) // inner)
    added = swapped(sent, inner)
    first = list(synthesis(direct, left_direct, None, shares, waves, None))
    first = exchanged(first, "freq")
    second = list(synthesis(paired, left_paired, added, shares, waves, lambda me: me // inner))
    second = exchanged(second, "freq")
    modelled = inverse(first, cas, waves, 0, groups, None)
    return inverse(second, cas, waves, 1, groups, modelled)


def start_order(size):
    return sorted(range(1, size), key=lambda shift: (abs(2 * shift - size), shift))


def solution(mesh):
    in_specs = (
        P("col", "freq", None, None),
        P("freq", None, "col", None, None),
        P("freq", None, "col", None, None),
        P("freq", None, "col"),
    )
    out_specs = P("col", "freq", None, None)
    return jax.shard_map(shards, mesh=mesh, in_specs=in_specs, out_specs=out_specs, check_vma=False)
```

```python
import functools

import jax
import jax.numpy as jnp
import numpy as np
from jax import lax
from jax.experimental import pallas as pl
from jax.experimental.pallas import tpu as pltpu
from jax.sharding import PartitionSpec as P

LANES = 128
WIDE = 58 << 20
ROWS = 16


def hartley_table(time_count, freq_count):
    phase = np.arange(time_count)[:, None] * np.arange(freq_count)[None, :] % time_count
    angle = np.float32(2.0 * np.pi / time_count) * phase.astype(np.float32)
    table = (np.cos(angle) + np.sin(angle)) / np.sqrt(np.float32(time_count))
    return table.astype(np.float32).astype(jnp.bfloat16)


def forward_kernel(x_ref, cas_ref, *refs, shares, depth, group):
    spectra, (buffer, held, arrived) = refs[:shares], refs[shares:]
    steps, pack, count, _, _ = buffer.shape
    all_freqs = cas_ref.shape[0]
    freqs = all_freqs // shares
    across = x_ref.shape[1] // count
    place = lax.axis_index("freq")

    def copies(step):
        first = pl.multiple_of(step % across * count, count)
        return [
            pltpu.make_async_copy(
                x_ref.at[step // across * pack + c, pl.ds(first, count)], buffer.at[step, c], arrived.at[step, c]
            )
            for c in range(pack)
        ]

    for step in range(min(depth, steps)):
        for copy in copies(step):
            copy.start()

    def body(step, carry):
        for copy in copies(step):
            copy.wait()

        @pl.when(step + depth < steps)
        def _():
            for copy in copies(step + depth):
                copy.start()

        for s in range(0, count, group):
            rows = jnp.concatenate([buffer[step, c, s + i] for i in range(group) for c in range(pack)], axis=0)
            product = lax.dot_general(
                cas_ref[...], rows, (((1,), (1,)), ((), ())), preferred_element_type=jnp.float32
            )
            for i in range(group):
                held[(s + i) * all_freqs : (s + i + 1) * all_freqs, :] = product[:, i * LANES : (i + 1) * LANES]
        first = pl.multiple_of(step % across * count, count)
        for shift in range(shares):
            low = lax.rem(place + shift, shares) * freqs
            for k in range(freqs):
                spectra[shift][k, step // across, pl.ds(first, count), :] = held[
                    pl.ds(low + k, count, stride=all_freqs), :
                ].astype(jnp.bfloat16)
        return carry

    lax.fori_loop(0, steps, body, 0)


def forward(traces, cas, shares):
    tiles, sources, waves, times = traces.shape
    all_freqs = cas.shape[0]
    freqs = all_freqs // shares
    pack = LANES // waves
    count = min(ROWS, sources)
    steps = tiles // pack * (sources // count)
    vmem = pl.BlockSpec(memory_space=pltpu.VMEM)
    return pl.pallas_call(
        functools.partial(forward_kernel, shares=shares, depth=4, group=4),
        out_shape=[jax.ShapeDtypeStruct((freqs, tiles // pack, sources, LANES), jnp.bfloat16)] * shares,
        in_specs=[pl.BlockSpec(memory_space=pltpu.HBM), vmem],
        out_specs=[vmem] * shares,
        scratch_shapes=[
            pltpu.VMEM((steps, pack, count, waves, times), jnp.bfloat16),
            pltpu.VMEM((count * all_freqs, LANES), jnp.float32),
            pltpu.SemaphoreType.DMA((steps, pack)),
        ],
        cost_estimate=pl.CostEstimate(
            flops=2 * traces.size * all_freqs, bytes_accessed=2 * traces.size, transcendentals=0
        ),
        name="forward",
    )(traces, cas)


def stage_kernel(*refs, count, pieces):
    operands, outputs, arrived = refs[:count], refs[count:-1], refs[-1]
    me = lax.axis_index("col")
    copies = [
        pltpu.make_async_copy(
            operands[operand] if take is None else operands[operand].at[:, pl.ds(take(me), wide)],
            outputs[output] if put is None else outputs[output].at[:, put],
            arrived.at[i],
        )
        for i, (operand, output, take, wide, put) in enumerate(pieces)
    ]
    for copy in copies:
        copy.start()
    for copy in copies:
        copy.wait()


def stage(operands, shapes, pieces, grant):
    return pl.pallas_call(
        functools.partial(stage_kernel, count=len(operands), pieces=pieces),
        out_shape=[jax.ShapeDtypeStruct(shape, jnp.bfloat16) for shape in shapes],
        in_specs=[pl.BlockSpec(memory_space=pltpu.HBM)] * len(operands),
        out_specs=[pl.BlockSpec(memory_space=pltpu.VMEM)] * len(shapes),
        scratch_shapes=[pltpu.SemaphoreType.DMA((len(pieces),))],
        cost_estimate=pl.CostEstimate(flops=1 << 28, bytes_accessed=1 << 22, transcendentals=0),
        compiler_params=pltpu.CompilerParams(vmem_limit_bytes=grant),
        name="stage",
    )(*operands)


def coeff_kernel(ranks_ref, right_ref, *refs, shares, owners, inner):
    spectra, direct = refs[:shares], refs[shares : shares + owners]
    paired, (spec_ref, rows_ref, right_held, spec_held, arrived) = refs[shares + owners : -5], refs[-5:]
    freqs, receivers, tiles, ranks, sources = right_ref.shape
    moves = [
        pltpu.make_async_copy(spectra[shift], spec_held.at[shift], arrived.at[freqs + shift])
        for shift in range(shares)
    ]
    for k in range(freqs):
        pltpu.make_async_copy(right_ref.at[k], right_held.at[k], arrived.at[k]).start()
        if k == 0:
            for move in moves:
                move.start()
    pairs, each = spectra[0].shape[1:3]
    pack = tiles // pairs
    waves = LANES // pack
    me, place = lax.axis_index("col"), lax.axis_index("freq")
    lane_tile = lax.broadcasted_iota(jnp.int32, (ranks, LANES), 1) // waves
    rank_row = lax.broadcasted_iota(jnp.int32, (ranks, LANES), 0)
    per_owner = receivers // owners

    for move in moves:
        move.wait()

    def body(k, carry):
        pltpu.make_async_copy(right_ref.at[k], right_held.at[k], arrived.at[k]).wait()
        for pair in range(pairs):
            for shift in range(shares):
                first = pl.multiple_of(lax.rem(place + shares - shift, shares) * each, each)
                spec_ref[pair, pl.ds(first, each), :] = spec_held[shift, k, pair]
        for pair in range(pairs):
            product = [
                jnp.dot(
                    right_held[k, :, pair * pack + h].reshape(receivers * ranks, sources),
                    spec_ref[pair],
                    preferred_element_type=jnp.float32,
                )
                for h in range(pack)
            ]
            for r in range(receivers):
                entry = (k * receivers + r) * tiles + pair * pack
                kept = product[0][r * ranks : (r + 1) * ranks]
                limit = jnp.full((ranks, LANES), ranks_ref[entry], jnp.int32)
                for h in range(1, pack):
                    here = lane_tile == h
                    kept = jnp.where(here, product[h][r * ranks : (r + 1) * ranks], kept)
                    limit = jnp.where(here, ranks_ref[entry + h], limit)
                kept = jnp.where(rank_row < limit, kept, 0.0)
                rows_ref[pair, r] = kept.astype(jnp.bfloat16)
            for shift in range(owners):
                first = lax.rem(me + shift, owners) * per_owner
                for i in range(pack):
                    direct[shift][k, pair, i * ranks : (i + 1) * ranks, :] = rows_ref[pair, first + i]
            for side in range(inner):
                core = lax.rem(me + side, inner)
                for outer in range(owners // inner):
                    first = (outer * inner + core) * per_owner + pack
                    for i in range(pack):
                        paired[side][k, outer, pair, i * ranks : (i + 1) * ranks, :] = rows_ref[pair, first + i]
        return carry

    lax.fori_loop(0, freqs, body, 0)


def coefficients(ranks, spectra, right, owners, inner):
    freqs, receivers, tiles, rank_count, sources = right.shape
    shares = len(spectra)
    pairs = spectra[0].shape[1]
    rows = tiles // pairs * rank_count
    outer = owners // inner
    vmem, smem = pl.BlockSpec(memory_space=pltpu.VMEM), pl.BlockSpec(memory_space=pltpu.SMEM)
    anywhere = pl.BlockSpec(memory_space=pl.ANY)
    return pl.pallas_call(
        functools.partial(coeff_kernel, shares=shares, owners=owners, inner=inner),
        out_shape=[jax.ShapeDtypeStruct((freqs, pairs, rows, LANES), jnp.bfloat16)] * owners
        + [jax.ShapeDtypeStruct((freqs, outer, pairs, rows, LANES), jnp.bfloat16)] * inner,
        in_specs=[smem, anywhere] + [anywhere] * shares,
        out_specs=[vmem] * (owners + inner),
        scratch_shapes=[
            pltpu.VMEM((pairs, sources, LANES), jnp.bfloat16),
            pltpu.VMEM((pairs, receivers, rank_count, LANES), jnp.bfloat16),
            pltpu.VMEM(right.shape, jnp.bfloat16),
            pltpu.VMEM((shares,) + spectra[0].shape, jnp.bfloat16),
            pltpu.SemaphoreType.DMA((freqs + shares,)),
        ],
        cost_estimate=pl.CostEstimate(
            flops=2 * right.size * LANES, bytes_accessed=2 * right.size, transcendentals=0
        ),
        compiler_params=pltpu.CompilerParams(vmem_limit_bytes=WIDE),
        name="coefficients",
    )(ranks.reshape(-1), right, *spectra)


def synthesis_kernel(*refs, count, chip, added):
    coeff_refs, left_refs = refs[:count], refs[count : 2 * count]
    freqs = left_refs[0].shape[0]
    pack, tiles, ranks, sources = left_refs[0].shape[-4:]
    waves = LANES // pack
    place = lax.axis_index("freq")
    here = None if chip is None else chip(lax.axis_index("col"))
    outputs = refs[2 * count + added :]
    turned = len(outputs) > 1
    if turned:
        outputs, turned_ref = outputs[:-1], outputs[-1]
        shares = len(outputs)
        each = sources // shares

    def pick(ref, k, rank):
        if len(ref.shape) == rank + 1:
            return ref.at[k]
        return ref.at[k, ref.shape[1] - 1 if here is None else here]

    for k in range(freqs):
        parts = []
        for r in range(pack):
            weights = jnp.concatenate(
                [
                    pick(ref, k, 3)[
                        c // pack, r * ranks : (r + 1) * ranks, c % pack * waves : (c % pack + 1) * waves
                    ]
                    for ref in coeff_refs
                    for c in range(tiles)
                ],
                axis=0,
            )
            left = jnp.concatenate([pick(ref, k, 4)[r].reshape(tiles * ranks, sources) for ref in left_refs], axis=0)
            part = lax.dot_general(weights, left, (((0,), (0,)), ((), ())), preferred_element_type=jnp.float32)
            if added:
                part = part + refs[2 * count][k, r].astype(jnp.float32)
            parts.append(part.astype(jnp.bfloat16))
        if turned:
            turned_ref[k] = jnp.concatenate(parts, axis=0).T
            for shift in range(shares):
                first = pl.multiple_of(lax.rem(place + shift, shares) * each, each)
                outputs[shift][k] = turned_ref[k, pl.ds(first, each), :]
        else:
            for r in range(pack):
                outputs[0][k, r] = parts[r]


def synthesis(coeffs, lefts, added, shares, waves, chip):
    pack = LANES // waves
    freqs = coeffs[0].shape[0]
    tiles, rank_count, sources = lefts[0].shape[-3:]
    vmem = pl.BlockSpec(memory_space=pltpu.VMEM)
    if shares:
        out_shape = [jax.ShapeDtypeStruct((freqs, sources // shares, LANES), jnp.bfloat16)] * shares
        scratch = [pltpu.VMEM((freqs, sources, LANES), jnp.bfloat16)]
    else:
        out_shape = [jax.ShapeDtypeStruct((freqs, pack, waves, sources), jnp.bfloat16)]
        scratch = []
    extra = [] if added is None else [added]
    flops = 2 * freqs * pack * waves * sources * tiles * rank_count * len(coeffs)
    return pl.pallas_call(
        functools.partial(synthesis_kernel, count=len(coeffs), chip=chip, added=len(extra)),
        out_shape=out_shape,
        in_specs=[vmem] * (2 * len(coeffs) + len(extra)),
        out_specs=[vmem] * len(out_shape),
        scratch_shapes=scratch,
        cost_estimate=pl.CostEstimate(flops=flops, bytes_accessed=flops // waves, transcendentals=0),
        compiler_params=pltpu.CompilerParams(vmem_limit_bytes=8 << 20),
        name="synthesis",
    )(*coeffs, *lefts, *extra)


def inverse_kernel(cas_ref, *refs, shares, group):
    syn_refs = refs[:shares]
    out_ref, buffer, held, left = refs[-4:]
    steps, pack, count, waves, _ = buffer.shape
    freqs = cas_ref.shape[0]
    rows = freqs // shares * count
    place = lax.axis_index("freq")

    def copies(step):
        first = pl.multiple_of(step * count, count)
        return [
            pltpu.make_async_copy(
                buffer.at[step, r], out_ref.at[group * pack + r, pl.ds(first, count)], left.at[step, r]
            )
            for r in range(pack)
        ]

    def body(step, carry):
        first = pl.multiple_of(step * count, count)
        for shift in range(shares):
            low = pl.multiple_of(lax.rem(place + shares - shift, shares) * rows, rows)
            held[pl.ds(low, rows), :] = (
                syn_refs[shift][:, pl.ds(first, count), :].astype(jnp.float32).reshape(rows, LANES)
            )
        for s in range(count):
            weights = held[pl.ds(s, freqs, stride=count), :].astype(jnp.bfloat16)
            block = lax.dot_general(
                weights, cas_ref[...], (((0,), (0,)), ((), ())), preferred_element_type=jnp.float32
            ).astype(jnp.bfloat16)
            for r in range(pack):
                buffer[step, r, s] = block[r * waves : (r + 1) * waves]
        for copy in copies(step):
            copy.start()
        return carry

    lax.fori_loop(0, steps, body, 0)
    for step in range(steps):
        for copy in copies(step):
            copy.wait()


def inverse(synthesised, cas, waves, group, groups, partial):
    shares = len(synthesised)
    _, sources, _ = synthesised[0].shape
    freqs, times = cas.shape
    pack = LANES // waves
    count = min(ROWS, sources)
    steps = sources // count
    vmem = pl.BlockSpec(memory_space=pltpu.VMEM)
    extra = [] if partial is None else [partial]
    return pl.pallas_call(
        functools.partial(inverse_kernel, shares=shares, group=group),
        out_shape=jax.ShapeDtypeStruct((groups * pack, sources, waves, times), jnp.bfloat16),
        in_specs=[vmem] + [vmem] * shares + [pl.BlockSpec(memory_space=pltpu.HBM)] * len(extra),
        out_specs=pl.BlockSpec(memory_space=pltpu.HBM),
        scratch_shapes=[
            pltpu.VMEM((steps, pack, count, waves, times), jnp.bfloat16),
            pltpu.VMEM((freqs * count, LANES), jnp.float32),
            pltpu.SemaphoreType.DMA((steps, pack)),
        ],
        input_output_aliases={1 + shares: 0} if extra else {},
        cost_estimate=pl.CostEstimate(
            flops=2 * sources * LANES * times * freqs,
            bytes_accessed=2 * sources * LANES * times,
            transcendentals=0,
        ),
        compiler_params=pltpu.CompilerParams(vmem_limit_bytes=14 << 20),
        name="inverse",
    )(cas, *synthesised, *extra)


def shards(traces, left_factors, right_factors, tile_ranks):
    shares, owners = lax.axis_size("freq"), lax.axis_size("col")
    inner = 2
    outer = owners // inner
    freq_local, receivers = left_factors.shape[:2]
    tile = left_factors.shape[2:]
    waves = traces.shape[2]
    pack = LANES // waves
    per_owner = receivers // owners
    groups = per_owner // pack
    cas = jnp.asarray(hartley_table(traces.shape[3], freq_local * shares).T)

    def shifted(block, shift, axis, size):
        return lax.ppermute(block, axis, [(i, (i + shift) % size) for i in range(size)])

    def exchanged(blocks, axis):
        size = len(blocks)
        arrived = [blocks[0]] + [None] * (size - 1)
        for shift in start_order(size):
            arrived[shift] = shifted(blocks[shift], shift, axis, size)
        return arrived

    def swapped(block, bit):
        return lax.ppermute(block, "col", [(i, i ^ bit) for i in range(owners)])

    made = list(forward(traces, cas, shares))

    def direct_first(shift):
        return lambda me: lax.rem(me + shift, owners) * per_owner

    def paired_first(side, chip):
        return lambda me: (chip * inner + lax.rem(me + side, inner)) * per_owner + pack

    direct_shape = (freq_local, pack) + tile
    paired_shape = (freq_local, outer, pack) + tile
    left_direct = stage(
        [left_factors],
        [direct_shape] * (owners - 1),
        [(0, shift - 1, direct_first(shift), pack, None) for shift in range(1, owners)],
        WIDE,
    )
    left_own, left_other = stage(
        [left_factors],
        [(freq_local, outer + 1, pack) + tile, paired_shape],
        [(0, side, paired_first(side, chip), pack, chip) for side in (1, 0) for chip in range(outer)]
        + [(0, 0, direct_first(0), pack, outer)],
        12 << 20,
    )
    spectra = exchanged(made, "freq")
    left_direct = exchanged([left_own] + list(left_direct), "col")
    left_paired = [left_own, swapped(left_other, 1)]

    made = list(coefficients(tile_ranks, spectra, right_factors, owners, inner))
    paired = [made[-2], swapped(made[-1], 1)]
    direct = exchanged(made[:owners], "col")
    (sent,) = synthesis(paired, left_paired, None, 0, waves, lambda me: (me ^ inner) // inner)
    added = swapped(sent, inner)
    first = list(synthesis(direct, left_direct, None, shares, waves, None))
    first = exchanged(first, "freq")
    second = list(synthesis(paired, left_paired, added, shares, waves, lambda me: me // inner))
    second = exchanged(second, "freq")
    modelled = inverse(first, cas, waves, 0, groups, None)
    return inverse(second, cas, waves, 1, groups, modelled)


def start_order(size):
    return sorted(range(1, size), key=lambda shift: (abs(2 * shift - size), shift))


def solution(mesh):
    in_specs = (
        P("col", "freq", None, None),
        P("freq", None, "col", None, None),
        P("freq", None, "col", None, None),
        P("freq", None, "col"),
    )
    out_specs = P("col", "freq", None, None)
    return jax.shard_map(shards, mesh=mesh, in_specs=in_specs, out_specs=out_specs, check_vma=False)
```
